32 devices in a mesh: dp: 4 (over x, core), seq: 8 (over z, y).
Axes of the slice: x: 2, y: 2, z: 4, core: 2. Of those that a mesh axis runs over, the one named last changes fastest.
Arguments:
- tokens: bfloat16 [8, 1152, 1280], P('dp', 'seq'), may hold values from -60 to 60
- pre_gain: float32 [1280], replicated, may hold values from 0.5 to 1.5
- pre_shift: float32 [1280], replicated, may hold values from -3 to 3
- w_qkv: bfloat16 [1280, 3840], P('dp'), may hold values from -4 to 4
- qkv_bias: float32 [3840], replicated, may hold values from -3 to 3
- w_out: bfloat16 [1280, 1280], P('dp'), may hold values from -0.15625 to 0.15625
- out_bias: float32 [1280], replicated, may hold values from -3 to 3
- mlp_gain: float32 [1280], replicated, may hold values from 0.5 to 1.5
- mlp_shift: float32 [1280], replicated, may hold values from -3 to 3
- w_up: bfloat16 [1280, 2560], P('dp'), may hold values from -0.15625 to 0.15625
- up_bias: float32 [2560], replicated, may hold values from -3 to 3
- w_down: bfloat16 [2560, 1280], P('dp'), may hold values from -0.125 to 0.125
- down_bias: float32 [1280], replicated, may hold values from -3 to 3
Outputs:
- layer_out: bfloat16 [8, 1152, 1280], P('dp', 'seq')
The draws below stay inside these ranges and needn't reach their ends.
All inputs are finite; a program needn't handle non-finite values.
Results may differ from the reference program's by a relative error of at most 0.0039.
Values may be sent and summed in bfloat16 or wider, within the bound.
A program may use at most 128 MiB of HBM per device.

```python
import math
import jax
import jax.numpy as jnp
from jax import lax

D = 1280
HEADS = 16
HEAD_DIM = 80
FF = 2560
IMAGES = 8
SEQ_LEN = 1152


def draw_tokens(key, part):
    subkeys = jax.random.split(jax.random.fold_in(key, 21), 4)
    shape = (IMAGES, SEQ_LEN, D)
    base = jax.random.normal(subkeys[0], shape, jnp.float32)
    row_scale = jnp.exp(jax.random.uniform(subkeys[2], (IMAGES, SEQ_LEN, 1), jnp.float32, math.log(0.4), math.log(4.0)))
    col_scale = jnp.exp(jax.random.uniform(subkeys[3], (1, 1, D), jnp.float32, math.log(0.4), math.log(4.0)))
    values = base * row_scale * col_scale
    return jnp.clip(values, -60.0, 60.0).astype(jnp.bfloat16)


def draw_w_qkv(key, part):
    subkey = jax.random.fold_in(key, 33)
    shape = (D, 3 * D)
    values = jnp.clip(jax.random.normal(subkey, shape, jnp.float32), -6.0, 6.0) / math.sqrt(D)
    return values.astype(jnp.bfloat16)


def block_levels(stream_key, extent, cuts, smallest, top_value):
    def one(axis_at, blocks):
        steps = jax.random.uniform(jax.random.fold_in(jax.random.fold_in(stream_key, 6), axis_at), (blocks,), jnp.float32, smallest / len(cuts), top_value / len(cuts))
        return jnp.repeat(jnp.exp(steps), extent[axis_at] // blocks).reshape((-1,) + (1,) * (len(extent) - axis_at - 1))

    level = one(*cuts[0])
    for cut in cuts[1:]:
        level = level * one(*cut)
    return level


def bell_draw(stream_key, extent, deviation, bound, cuts=(), held_as=jnp.bfloat16):
    array = jax.random.normal(stream_key, extent, jnp.float32) * deviation
    if len(cuts) > 0:
        array = block_levels(stream_key, extent, cuts, -0.22, 0.18) * array
    return jnp.clip(array, min=-bound, max=bound).astype(held_as)


def setup_inputs(seed: int = 0) -> dict:
    key_of = jax.random.split(jax.random.key(seed), 14)
    return {
        "tokens": draw_tokens(jax.random.fold_in(key_of[13], 71), 0),
        "pre_gain": jnp.clip(1.0 + 0.1 * jax.random.normal(key_of[1], (D,), jnp.float32), 0.5, 1.5),
        "pre_shift": bell_draw(key_of[2], (D,), 0.5, 3.0, (), jnp.float32),
        "w_qkv": draw_w_qkv(jax.random.fold_in(key_of[13], 71), 0),
        "qkv_bias": bell_draw(key_of[4], (3 * D,), 0.5, 3.0, (), jnp.float32),
        "w_out": bell_draw(key_of[5], (D, D), D ** -0.5, 0.15625, ((0, 4),)),
        "out_bias": bell_draw(key_of[6], (D,), 0.5, 3.0, (), jnp.float32),
        "mlp_gain": jnp.clip(1.0 + 0.1 * jax.random.normal(key_of[7], (D,), jnp.float32), 0.5, 1.5),
        "mlp_shift": bell_draw(key_of[8], (D,), 0.5, 3.0, (), jnp.float32),
        "w_up": bell_draw(key_of[9], (D, FF), D ** -0.5, 0.15625, ((0, 4),)),
        "up_bias": bell_draw(key_of[10], (FF,), 0.5, 3.0, (), jnp.float32),
        "w_down": bell_draw(key_of[11], (FF, D), FF ** -0.5, 0.125, ((0, 4),)),
        "down_bias": bell_draw(key_of[12], (D,), 0.5, 3.0, (), jnp.float32),
    }


EPSILON = 1e-05

def normalize(features, gain, shift):
    average = lax.optimization_barrier(jnp.mean(features, axis=-1, keepdims=True))
    centered = features - average
    spread = lax.optimization_barrier(jnp.mean(centered * centered, axis=-1, keepdims=True))
    return centered * lax.rsqrt(spread + EPSILON) * gain + shift

def attend_head(packed_head):
    queries = packed_head[:, :HEAD_DIM]
    key_rows = packed_head[:, HEAD_DIM:2 * HEAD_DIM]
    value_rows = packed_head[:, 2 * HEAD_DIM:]
    scores = jnp.dot(queries, key_rows.T, preferred_element_type=jnp.float32) * (1.0 / math.sqrt(HEAD_DIM))
    highest = lax.optimization_barrier(jnp.max(scores, axis=-1, keepdims=True))
    weights = jnp.exp(scores - highest)
    probs = (weights / lax.optimization_barrier(jnp.sum(weights, axis=-1, keepdims=True))).astype(jnp.bfloat16)
    return jnp.dot(probs, value_rows, preferred_element_type=jnp.float32).astype(jnp.bfloat16)

def reference(tokens, pre_gain, pre_shift, w_qkv, qkv_bias, w_out, out_bias, mlp_gain, mlp_shift, w_up, up_bias, w_down, down_bias):

    def one_picture(picture):
        residual = picture.astype(jnp.float32)
        normed = normalize(residual, pre_gain, pre_shift).astype(jnp.bfloat16)
        packed = (jnp.dot(normed, w_qkv, preferred_element_type=jnp.float32) + qkv_bias).astype(jnp.bfloat16)
        per_head = packed.reshape(SEQ_LEN, HEADS, 3 * HEAD_DIM).transpose(1, 0, 2)
        context = lax.map(attend_head, per_head)
        context = context.transpose(1, 0, 2).reshape(SEQ_LEN, D)
        middle = residual + jnp.dot(context, w_out, preferred_element_type=jnp.float32) + out_bias
        normed_mlp = normalize(middle, mlp_gain, mlp_shift).astype(jnp.bfloat16)
        lifted = jnp.dot(normed_mlp, w_up, preferred_element_type=jnp.float32) + up_bias
        hidden = jax.nn.gelu(lifted, approximate=False).astype(jnp.bfloat16)
        lowered = jnp.dot(hidden, w_down, preferred_element_type=jnp.float32)
        return (middle + lowered + down_bias).astype(jnp.bfloat16)
    return lax.map(one_picture, tokens)
```

```python
import functools
import math

import jax
import jax.numpy as jnp
from jax import lax
from jax.experimental import pallas as pl
from jax.experimental.pallas import tpu as pltpu
from jax.sharding import PartitionSpec as P

HEADS = 16
HEAD_DIM = 80
LANES = 128
EPSILON = 1e-05
MESH = pl.DeviceIdType.MESH
HALF = jnp.bfloat16
NORM_ROWS = 48


def up_to(value, step):
    return -(-value // step) * step


class Plan:
    def __init__(self, n, n_dp, images, tok, width, hidden, qkv_width):
        self.n, self.n_dp, self.images, self.tok = n, n_dp, images, tok
        self.width, self.hidden, self.qkv_width = width, hidden, qkv_width
        self.pairs = n_dp // 2
        self.groups = 2 * images
        self.across = n // self.groups
        self.heads = HEADS // (2 * self.across)
        self.length = n * tok
        self.part_heads = self.heads // 2
        self.span = self.part_heads * HEAD_DIM
        self.part_columns = self.part_heads * 3 * LANES
        columns = self.heads * 3 * HEAD_DIM
        starts = [g * columns for g in range(2 * self.across)]
        rest = max(start % LANES for start in starts)
        self.window = up_to(rest + columns, LANES)
        last = starts[-1] // LANES * LANES
        self.shift_back = max(0, last + self.window - qkv_width)
        firsts = [start // LANES * LANES for start in starts]
        firsts[-1] -= self.shift_back
        self.rests = [start - first for start, first in zip(starts, firsts)]
        self.columns = columns
        cut = min(self.window, up_to(max(self.rests) + columns // 2, LANES))
        self.cuts = (0, cut, self.window) if cut < self.window else (0, cut)
        self.q_rows = width // n_dp


def normalize(features, gain, shift):
    average = jnp.mean(features, axis=-1, keepdims=True)
    centered = features - average
    spread = jnp.mean(centered * centered, axis=-1, keepdims=True)
    return centered * lax.rsqrt(spread + EPSILON) * gain + shift


def pieces_of(plan):
    half_out, half_up = plan.width // 2, plan.hidden // 2
    cut = up_to(half_out // 2, LANES)
    return (
        (0, 0, half_out, 0),
        (1, 0, half_up // 2, 0),
        (1, half_up // 2, half_up // 2, 0),
        (2, 0, cut, 1),
        (2, cut, half_out - cut, 1),
    )


def layer_kernel(
    plan,
    tok_ref,
    wq_ref,
    wo_ref,
    wu_ref,
    wd_ref,
    pg_ref,
    ps_ref,
    qb_ref,
    ob_ref,
    mg_ref,
    ms_ref,
    ub_ref,
    db_ref,
    o_ref,
    xin,
    xn,
    wraw,
    wbuf,
    bpad,
    packed,
    mixed,
    landed,
    ctx,
    mid,
    hid,
    w_out,
    w_up,
    w_down,
    t_send,
    t_recv,
    ty_send,
    ty_recv,
    ts_send,
    ts_recv,
    q_send,
    q_recv,
    qz_send,
    qz_recv,
    qs_send,
    qs_recv,
    q_own,
    x_send,
    x_recv,
    p_send,
    p_recv,
    s_send,
    s_recv,
    so_send,
    so_recv,
    own_sem,
    c_send,
    c_recv,
):
    n, n_dp, images, tok = plan.n, plan.n_dp, plan.images, plan.tok
    groups, across, pairs = plan.groups, plan.across, plan.pairs
    d, s = lax.axis_index("dp"), lax.axis_index("seq")
    core = d % 2
    pair = d // 2
    sibling = d + 1 - 2 * core
    z, y = s // across, s % across
    z_near = z + 1 - 2 * (z % 2)
    y_near = y + 1 - 2 * (y % 2)
    z_order = (z, z_near, (z + 2) % groups, (z_near + 2) % groups)
    mine = z // images == core
    others = z // images != core
    shards_of = (wo_ref, wu_ref, wd_ref)
    wholes = (w_out, w_up, w_down)
    pieces = pieces_of(plan)
    n_parts = len(plan.cuts) - 1
    factor = math.log2(math.e) / math.sqrt(HEAD_DIM)

    barrier = pltpu.get_barrier_semaphore()
    for t in range(n):
        if t:
            pl.semaphore_signal(barrier, inc=1, device_id=(d, (s + t) % n), device_id_type=MESH)
        pl.semaphore_signal(barrier, inc=1, device_id=(sibling, (s + t) % n), device_id_type=MESH)
    for j in range(1, pairs):
        for cc in range(2):
            there = (pair + j) % pairs * 2 + cc
            pl.semaphore_signal(barrier, inc=1, device_id=(there, s), device_id_type=MESH)
    pl.semaphore_wait(barrier, 2 * n - 1 + 2 * (pairs - 1))

    def remote(src, dst, send, recv, device):
        return pltpu.make_async_remote_copy(
            src_ref=src, dst_ref=dst, send_sem=send, recv_sem=recv, device_id=device, device_id_type=MESH
        )

    def token_z(i):
        there = core * images + i
        return remote(tok_ref.at[i], xin.at[s], t_send.at[i], t_recv.at[z], (d, there * across + y))

    def token_z_in(zp):
        slot = xin.at[zp * across + y]
        return remote(slot, slot, t_send.at[0], t_recv.at[zp], (d, s))

    def token_y(zp, dy, src):
        there = z * across + (y + dy) % across
        return remote(src, xin.at[zp * across + y], ty_send.at[zp, dy], ty_recv.at[zp, dy], (d, there))

    def token_y_in(zp, dy):
        slot = xin.at[zp * across + (y + across - dy) % across]
        return remote(slot, slot, ty_send.at[zp, dy], ty_recv.at[zp, dy], (d, s))

    def token_s(sp, src):
        return remote(src, xin.at[sp], ts_send.at[sp], ts_recv.at[sp], (sibling, s))

    def own_tokens():
        return tok_ref.at[z % images]

    def q_first(group):
        return pl.multiple_of(
            group * plan.columns // LANES * LANES - group // (2 * across - 1) * plan.shift_back, LANES
        )

    def q_columns(part, group):
        low, high = plan.cuts[part], plan.cuts[part + 1]
        return pl.ds(pl.multiple_of(q_first(group) + low, LANES), high - low)

    def q_part(part):
        return pl.ds(plan.cuts[part], plan.cuts[part + 1] - plan.cuts[part])

    q_half = plan.q_rows // 2

    def q_slab(owner, half):
        return pl.ds(pl.multiple_of(owner * plan.q_rows + half * q_half, 8), q_half)

    def q_x(part, j, cc):
        half = z % 2
        return remote(
            wq_ref.at[pl.ds(pl.multiple_of(half * q_half, 8), q_half), q_columns(part, 2 * y + cc)],
            wraw.at[q_slab(d, half), q_part(part)],
            q_send.at[part, j, cc],
            q_recv.at[part, j, core],
            ((pair + j) % pairs * 2 + cc, s),
        )

    def q_x_in(part, j, cc):
        slot = wraw.at[q_slab((pair + pairs - j) % pairs * 2 + cc, z % 2), q_part(part)]
        return remote(slot, slot, q_send.at[part, j, cc], q_recv.at[part, j, cc], (d, s))

    def q_z(part, j, cc, arriving=False):
        half = 1 - z % 2 if arriving else z % 2
        slot = wraw.at[q_slab((pair + pairs - j) % pairs * 2 + cc, half), q_part(part)]
        there = z_near * across + y
        return remote(slot, slot, qz_send.at[part, j, cc], qz_recv.at[part, j, cc], (d, there))

    def q_full(owner):
        return pl.ds(pl.multiple_of(owner * plan.q_rows, 16), plan.q_rows)

    def q_s(part, arriving=False):
        return remote(
            wq_ref.at[:, q_columns(part, 2 * y + 1 - core)],
            wraw.at[q_full(sibling if arriving else d), q_part(part)],
            qs_send.at[part],
            qs_recv.at[part],
            (sibling, s),
        )

    def q_mine(part):
        return pltpu.make_async_copy(
            wq_ref.at[:, q_columns(part, 2 * y + core)], wraw.at[q_full(d), q_part(part)], q_own.at[part]
        )

    def slab(k, owner):
        depth = shards_of[k].shape[0]
        return pl.ds(pl.multiple_of(owner * depth, 16), depth)

    def piece_columns(piece, other=False):
        k, low, columns, along_z = piece
        half = z % 2 if along_z else y % 2
        if other:
            half = 1 - half
        return pl.ds(pl.multiple_of(half * (wholes[k].shape[1] // 2) + low, LANES), columns)

    def owner_of(j):
        return (pair + pairs - j) % pairs * 2 + core

    def w_x(q, j, arriving=False):
        k = pieces[q][0]
        columns = piece_columns(pieces[q])
        return remote(
            shards_of[k].at[:, columns],
            wholes[k].at[slab(k, owner_of(j) if arriving else d), columns],
            x_send.at[q, j],
            x_recv.at[q, j],
            ((pair + j) % pairs * 2 + core, s),
        )

    def w_p(q, j, arriving=False):
        k, along_z = pieces[q][0], pieces[q][3]
        slot = wholes[k].at[slab(k, owner_of(j)), piece_columns(pieces[q], arriving)]
        there = z_near * across + y if along_z else z * across + y_near
        return remote(slot, slot, p_send.at[q, j], p_recv.at[q, j], (d, there))

    def w_s(q, j, second, arriving=False):
        k = pieces[q][0]
        owner = (pair + pairs - j) % pairs * 2 + (1 - core if arriving else core)
        slot = wholes[k].at[slab(k, owner), piece_columns(pieces[q], second)]
        way = 1 if second else 0
        return remote(slot, slot, s_send.at[q, j, way], s_recv.at[q, j, way], (sibling, s))

    def w_so(k, arriving=False):
        return remote(
            shards_of[k],
            wholes[k].at[slab(k, sibling if arriving else d)],
            so_send.at[k],
            so_recv.at[k],
            (sibling, s),
        )

    def w_own(k):
        return pltpu.make_async_copy(shards_of[k], wholes[k].at[slab(k, d)], own_sem.at[k])

    def pass_first(q):
        for j in range(1, pairs):
            w_x(q, j, True).wait_recv()
            w_p(q, j).start()
            w_s(q, j, False).start()

    def pass_second(q):
        for j in range(1, pairs):
            w_p(q, j, True).wait_recv()
            w_s(q, j, True).start()

    def arrived(k):
        w_own(k).wait()
        w_so(k, True).wait_recv()
        for q, piece in enumerate(pieces):
            if piece[0] == k:
                for j in range(1, pairs):
                    for second in (False, True):
                        w_s(q, j, second, True).wait_recv()

    def ctx_copy(part, sp, group, slot):
        return remote(
            mixed.at[part, sp],
            landed.at[part, group, slot],
            c_send.at[part, sp],
            c_recv.at[part, group, slot],
            (pair * 2 + z // images, sp),
        )

    for k in range(images):
        i = (1 - core) * k + core * (images - 1 - k)

        @pl.when(core * images + i != z)
        def _():
            token_z(i).start()

    @pl.when(mine)
    def _():
        for dy in range(1, across):
            token_y(z, dy, own_tokens()).start()
        token_s(s, own_tokens()).start()

    for part in range(n_parts):
        for j in range(1, pairs):
            q_x(part, j, 0).start()
            q_x(part, j, 1).start()
    for part in range(n_parts):
        q_mine(part).start()
        q_s(part).start()
    for q in range(len(pieces)):
        for j in range(1, pairs):
            w_x(q, j).start()

    wbuf[...] = jnp.zeros_like(wbuf)
    group = 2 * y + core
    per_part = plan.part_heads * 3
    for rest in sorted(set(plan.rests)):
        which = [g for g, r in enumerate(plan.rests) if r == rest]
        hit = group == which[0]
        for g in which[1:]:
            hit = jnp.logical_or(hit, group == g)

        @pl.when(hit)
        def _(rest=rest):
            row = qb_ref[:, pl.ds(q_first(group), plan.window)]
            for g in range(2 * per_part):
                piece = row[:, rest + g * HEAD_DIM : rest + (g + 1) * HEAD_DIM]
                at = g % per_part * LANES
                ones = jnp.full((1, LANES - HEAD_DIM), 1.0 if g % 3 == 2 else 0.0, jnp.float32)
                bpad[g // per_part, :, at : at + LANES] = jnp.concatenate([piece, ones], axis=-1)

    def norm_block(zp):
        rows = across * tok

        def chunk(i, carry):
            at = pl.ds(pl.multiple_of(zp * rows + i * NORM_ROWS, 16), NORM_ROWS)
            per = tok // NORM_ROWS
            inside = pl.ds(pl.multiple_of(i % per * NORM_ROWS, 16), NORM_ROWS)
            block = xin[zp * across + i // per, inside, :].astype(jnp.float32)
            xn[at, :] = normalize(block, pg_ref[...], ps_ref[...]).astype(HALF)
            return carry

        lax.fori_loop(0, rows // NORM_ROWS, chunk, 0)

    @pl.when(mine)
    def _():
        xin[s] = tok_ref[z % images]
        for dy in range(1, across):
            token_y_in(z, dy).wait_recv()
            slot = z * across + (y + across - dy) % across
            token_s(slot, xin.at[slot]).start()

    @pl.when(others)
    def _():
        for yy in range(across):
            slot = z * across + yy
            token_s(slot, xin.at[slot]).wait_recv()

    norm_block(z)
    for step in range(1, groups):
        zp = z_order[step]
        slot = zp * across + y

        @pl.when(mine)
        def _():
            token_z_in(zp).wait_recv()
            for dy in range(1, across):
                token_y(zp, dy, xin.at[slot]).start()
            token_s(slot, xin.at[slot]).start()

        if step - 1 < n_parts:
            for j in range(1, pairs):
                for cc in range(2):
                    q_x_in(step - 1, j, cc).wait_recv()
                    q_z(step - 1, j, cc).start()

        def finish(zq):
            @pl.when(mine)
            def _():
                for dy in range(1, across):
                    token_y_in(zq, dy).wait_recv()
                    other = zq * across + (y + across - dy) % across
                    token_s(other, xin.at[other]).start()

            @pl.when(others)
            def _():
                for yy in range(across):
                    one = zq * across + yy
                    token_s(one, xin.at[one]).wait_recv()

            norm_block(zq)

        if step > 1:
            finish(z_order[step - 1])
        if step == groups - 1:
            finish(zp)

    for k in range(3):
        w_own(k).start()
        w_so(k).start()

    def build(part):
        q_mine(part).wait()
        q_s(part, True).wait_recv()
        for j in range(1, pairs):
            for cc in range(2):
                q_z(part, j, cc, True).wait_recv()

    def pad_weights(part):
        for rest in sorted(set(plan.rests)):
            which = [g for g, r in enumerate(plan.rests) if r == rest]
            hit = group == which[0]
            for g in which[1:]:
                hit = jnp.logical_or(hit, group == g)

            @pl.when(hit)
            def _(rest=rest):
                for g in range(per_part):
                    low = rest + (part * per_part + g) * HEAD_DIM
                    wbuf[part, :, g * LANES : g * LANES + HEAD_DIM] = wraw[:, low : low + HEAD_DIM]

    block_rows = across * tok

    def project(part):
        def one(i, carry):
            at = pl.ds(pl.multiple_of(i * block_rows, 16), block_rows)
            result = jnp.dot(xn[at, :], wbuf[part], preferred_element_type=jnp.float32) + bpad[part]
            packed[part, at, :] = result.astype(HALF)
            return carry

        lax.fori_loop(0, groups, one, 0)

    def attend(part, after):
        def one(step, carry):
            near = (step + 1) // 2 % 2
            far = 1 - step // 2
            zp = (z + near * (1 - 2 * (z % 2)) + 2 * far) % groups
            at = pl.ds(pl.multiple_of(zp * block_rows, 16), block_rows)
            outs = []
            for h in range(plan.part_heads):
                base = h * 3 * LANES
                queries = packed[part, at, base : base + LANES]
                key_rows = packed[part, :, base + LANES : base + 2 * LANES]
                value_rows = packed[part, :, base + 2 * LANES : base + 3 * LANES]
                scores = lax.dot_general(
                    queries, key_rows, (((1,), (1,)), ((), ())), preferred_element_type=jnp.float32
                )
                highest = jnp.max(scores, axis=-1, keepdims=True)
                weights = jnp.exp2((scores - highest) * factor).astype(HALF)
                summed = jnp.dot(weights, value_rows, preferred_element_type=jnp.float32)
                outs.append(summed[:, :HEAD_DIM] / summed[:, HEAD_DIM : HEAD_DIM + 1])
            whole = (jnp.concatenate(outs, axis=-1) if len(outs) > 1 else outs[0]).astype(HALF)
            for yy in range(across):
                sp = zp * across + yy
                mixed[part, sp] = whole[yy * tok : (yy + 1) * tok]
                own = jnp.logical_and(mine, sp == s)

                @pl.when(own)
                def _():
                    landed[part, group, z % images] = whole[yy * tok : (yy + 1) * tok]

                @pl.when(jnp.logical_not(own))
                def _():
                    ctx_copy(part, sp, group, z % images).start()

            for when, action in after:

                @pl.when(step == when)
                def _():
                    action()

            return carry

        lax.fori_loop(0, groups, one, 0)

    build(0)
    pad_weights(0)
    project(0)
    pass_first(0)
    attend(0, [(1, lambda: pass_second(0))])
    build(1)
    pad_weights(1)
    project(1)
    pass_first(1)
    attend(1, [(2, lambda: pass_second(1))])

    pass_first(2)

    def context_in(part, gg, i):
        yy, cc = gg // 2, gg % 2
        source = (core * images + i) * across + yy
        own = jnp.logical_and(source == s, core == cc)
        slot = landed.at[part, gg, i]

        @pl.when(jnp.logical_not(own))
        def _():
            remote(
                mixed.at[part, 0], slot, c_send.at[part, 0], c_recv.at[part, gg, i], (pair * 2 + cc, source)
            ).wait_recv()

    for part in range(2):
        for i in range(images):
            for gg in range(2 * across):
                context_in(part, gg, i)
                low = gg * plan.heads * HEAD_DIM + part * plan.span
                ctx[i * tok : (i + 1) * tok, low : low + plan.span] = landed[part, gg, i]

    pass_second(2)
    arrived(0)
    row_count = images * tok

    def tile_of(c):
        return pl.ds(pl.multiple_of(c * 2 * LANES, 2 * LANES), 2 * LANES)

    def out_tile(c, carry):
        cols = tile_of(c)
        attended = jnp.dot(ctx[...], w_out[:, cols], preferred_element_type=jnp.float32)
        residual = tok_ref[:, :, cols].astype(jnp.float32).reshape(row_count, 2 * LANES)
        mid[:, cols] = residual + attended + ob_ref[:, cols]
        return carry

    lax.fori_loop(0, plan.width // (2 * LANES), out_tile, 0)

    def second_norm(i, carry):
        at = pl.ds(pl.multiple_of(i * NORM_ROWS, 16), NORM_ROWS)
        ctx[at, :] = normalize(mid[at, :], mg_ref[...], ms_ref[...]).astype(HALF)
        return carry

    lax.fori_loop(0, row_count // NORM_ROWS, second_norm, 0)
    arrived(1)

    def up_tile(c, carry):
        cols = tile_of(c)
        lifted = jnp.dot(ctx[...], w_up[:, cols], preferred_element_type=jnp.float32)
        lifted = lifted + ub_ref[:, cols]
        hid[:, cols] = (0.5 * lifted * (1.0 + lax.erf(lifted * math.sqrt(0.5)))).astype(HALF)
        return carry

    lax.fori_loop(0, plan.hidden // (2 * LANES), up_tile, 0)
    pass_first(3)
    pass_first(4)
    pass_second(3)
    pass_second(4)
    arrived(2)

    def down_tile(c, carry):
        cols = tile_of(c)
        lowered = jnp.dot(hid[...], w_down[:, cols], preferred_element_type=jnp.float32)
        result = (mid[:, cols] + lowered + db_ref[:, cols]).astype(HALF)
        o_ref[:, :, cols] = result.reshape(images, tok, 2 * LANES)
        return carry

    lax.fori_loop(0, plan.width // (2 * LANES), down_tile, 0)

    for k in range(images):

        @pl.when(core * images + k != z)
        def _():
            token_z(k).wait_send()

    @pl.when(mine)
    def _():
        for zp in range(groups):
            slot = zp * across + y
            for dy in range(1, across):
                token_y(zp, dy, xin.at[slot]).wait_send()
        for sp in range(n):
            token_s(sp, xin.at[sp]).wait_send()

    for part in range(n_parts):
        q_s(part).wait_send()
        for j in range(1, pairs):
            for cc in range(2):
                q_x(part, j, cc).wait_send()
                q_z(part, j, cc).wait_send()
    for k in range(3):
        w_so(k).wait_send()
    for q in range(len(pieces)):
        for j in range(1, pairs):
            w_x(q, j).wait_send()
            w_p(q, j).wait_send()
            w_s(q, j, False).wait_send()
            w_s(q, j, True).wait_send()
    for part in range(2):
        for sp in range(n):

            @pl.when(jnp.logical_not(jnp.logical_and(mine, sp == s)))
            def _():
                ctx_copy(part, sp, group, z % images).wait_send()


def shards(n, n_dp, tokens, pre_gain, pre_shift, w_qkv, qkv_bias, w_out, out_bias, mlp_gain, mlp_shift,
           w_up, up_bias, w_down, down_bias):
    images, tok, width = tokens.shape
    hidden = w_up.shape[1]
    plan = Plan(n, n_dp, images, tok, width, hidden, w_qkv.shape[1])
    rows = images * tok
    dma = pltpu.SemaphoreType.DMA
    vmem = pl.BlockSpec(memory_space=pltpu.VMEM)
    anywhere = pl.BlockSpec(memory_space=pl.ANY)
    pairs, groups, across = plan.pairs, plan.groups, plan.across
    n_pieces = len(pieces_of(plan))
    parts = len(plan.cuts) - 1
    return pl.pallas_call(
        functools.partial(layer_kernel, plan),
        out_shape=jax.ShapeDtypeStruct(tokens.shape, HALF),
        in_specs=[vmem] + [anywhere] * 4 + [vmem] * 8,
        out_specs=vmem,
        scratch_shapes=[
            pltpu.VMEM((n, tok, width), HALF),
            pltpu.VMEM((plan.length, width), HALF),
            pltpu.VMEM((width, plan.window), HALF),
            pltpu.VMEM((2, width, plan.part_columns), HALF),
            pltpu.VMEM((2, 1, plan.part_columns), jnp.float32),
            pltpu.VMEM((2, plan.length, plan.part_columns), HALF),
            pltpu.VMEM((2, n, tok, plan.span), HALF),
            pltpu.VMEM((2, 2 * across, images, tok, plan.span), HALF),
            pltpu.VMEM((rows, width), HALF),
            pltpu.VMEM((rows, width), jnp.float32),
            pltpu.VMEM((rows, hidden), HALF),
            pltpu.VMEM((width, width), HALF),
            pltpu.VMEM((width, hidden), HALF),
            pltpu.VMEM((hidden, width), HALF),
            dma((images,)),
            dma((groups,)),
            dma((groups, across)),
            dma((groups, across)),
            dma((n,)),
            dma((n,)),
            dma((parts, pairs, 2)),
            dma((parts, pairs, 2)),
            dma((parts, pairs, 2)),
            dma((parts, pairs, 2)),
            dma((parts,)),
            dma((parts,)),
            dma((parts,)),
            dma((n_pieces, pairs)),
            dma((n_pieces, pairs)),
            dma((n_pieces, pairs)),
            dma((n_pieces, pairs)),
            dma((n_pieces, pairs, 2)),
            dma((n_pieces, pairs, 2)),
            dma((3,)),
            dma((3,)),
            dma((3,)),
            dma((2, n)),
            dma((2, 2 * across, images)),
        ],
        compiler_params=pltpu.CompilerParams(
            collective_id=0, has_side_effects=True, vmem_limit_bytes=60 * 1024 * 1024
        ),
        name="encoder_layer",
    )(
        tokens,
        w_qkv,
        w_out,
        w_up,
        w_down,
        pre_gain[None],
        pre_shift[None],
        qkv_bias[None],
        out_bias[None],
        mlp_gain[None],
        mlp_shift[None],
        up_bias[None],
        down_bias[None],
    )


def solution(mesh):
    in_specs = (
        P("dp", "seq", None),
        P(),
        P(),
        P("dp", None),
        P(),
        P("dp", None),
        P(),
        P(),
        P(),
        P("dp", None),
        P(),
        P("dp", None),
        P(),
    )
    out_specs = P("dp", "seq", None)
    step = functools.partial(shards, mesh.shape["seq"], mesh.shape["dp"])
    return jax.shard_map(step, mesh=mesh, in_specs=in_specs, out_specs=out_specs, check_vma=False)
```

```python
import functools
import math

import jax
import jax.numpy as jnp
from jax import lax
from jax.experimental import pallas as pl
from jax.experimental.pallas import tpu as pltpu
from jax.sharding import PartitionSpec as P

HEADS = 16
HEAD_DIM = 80
LANES = 128
EPSILON = 1e-05
MESH = pl.DeviceIdType.MESH
HALF = jnp.bfloat16
NORM_ROWS = 48


def up_to(value, step):
    return -(-value // step) * step


class Plan:
    def __init__(self, n, n_dp, images, tok, width, hidden, qkv_width):
        self.n, self.n_dp, self.images, self.tok = n, n_dp, images, tok
        self.width, self.hidden, self.qkv_width = width, hidden, qkv_width
        self.pairs = n_dp // 2
        self.groups = 2 * images
        self.across = n // self.groups
        self.heads = HEADS // (2 * self.across)
        self.length = n * tok
        self.part_heads = self.heads // 2
        self.span = self.part_heads * HEAD_DIM
        early = self.span // LANES * LANES
        self.sends = ((0, early), (early, 2 * self.span))
        self.part_columns = self.part_heads * 3 * LANES
        columns = self.heads * 3 * HEAD_DIM
        starts = [g * columns for g in range(2 * self.across)]
        rest = max(start % LANES for start in starts)
        self.window = up_to(rest + columns, LANES)
        last = starts[-1] // LANES * LANES
        self.shift_back = max(0, last + self.window - qkv_width)
        firsts = [start // LANES * LANES for start in starts]
        firsts[-1] -= self.shift_back
        self.rests = [start - first for start, first in zip(starts, firsts)]
        self.columns = columns
        cut = min(self.window, up_to(max(self.rests) + columns // 2, LANES))
        self.cuts = (0, cut, self.window) if cut < self.window else (0, cut)
        self.q_rows = width // n_dp


def normalize(features, gain, shift):
    average = jnp.mean(features, axis=-1, keepdims=True)
    centered = features - average
    spread = jnp.mean(centered * centered, axis=-1, keepdims=True)
    return centered * lax.rsqrt(spread + EPSILON) * gain + shift


def thirds(columns, parts):
    tiles = columns // LANES
    sizes = [(tiles + parts - 1 - p) // parts * LANES for p in range(parts)]
    return [(sum(sizes[:p]), size) for p, size in enumerate(sizes) if size]


def pieces_of(plan):
    cuts = (thirds(plan.width // 2, 1), thirds(plan.hidden // 2, 4), thirds(plan.width // 2, 3))
    along = ((0,), (0, 0, 0, 1), (1, 0, 1))
    return tuple((k, low, size, along[k][p]) for k in range(3) for p, (low, size) in enumerate(cuts[k]))


def layer_kernel(
    plan,
    tok_in,
    wq_ref,
    wo_ref,
    wu_ref,
    wd_ref,
    pg_in,
    ps_in,
    qb_in,
    ob_in,
    mg_in,
    ms_in,
    ub_in,
    db_in,
    o_out,
    tok_ref,
    o_ref,
    io_sem,
    pg_ref,
    ps_ref,
    qb_ref,
    ob_ref,
    mg_ref,
    ms_ref,
    ub_ref,
    db_ref,
    vec_sem,
    xin,
    xn,
    wraw,
    wbuf,
    bpad,
    packed,
    mixed,
    landed,
    ctx,
    mid,
    hid,
    w_out,
    w_up,
    w_down,
    t_send,
    t_recv,
    ty_send,
    ty_recv,
    ts_send,
    ts_recv,
    q_send,
    q_recv,
    qz_send,
    qz_recv,
    qs_send,
    qs_recv,
    q_own,
    x_send,
    x_recv,
    p_send,
    p_recv,
    s_send,
    s_recv,
    so_send,
    so_recv,
    own_sem,
    c_send,
    c_recv,
):
    n, n_dp, images, tok = plan.n, plan.n_dp, plan.images, plan.tok
    groups, across, pairs = plan.groups, plan.across, plan.pairs
    d, s = lax.axis_index("dp"), lax.axis_index("seq")
    core = d % 2
    pair = d // 2
    sibling = d + 1 - 2 * core
    z, y = s // across, s % across
    z_near = z + 1 - 2 * (z % 2)
    y_near = y + 1 - 2 * (y % 2)
    z_order = (z, z_near, (z + 2) % groups, (z_near + 2) % groups)
    mine = z // images == core
    others = z // images != core
    shards_of = (wo_ref, wu_ref, wd_ref)
    wholes = (w_out, w_up, w_down)
    pieces = pieces_of(plan)
    n_parts = len(plan.cuts) - 1
    factor = math.log2(math.e) / math.sqrt(HEAD_DIM)

    vectors = ((pg_in, pg_ref), (ps_in, ps_ref), (qb_in, qb_ref), (ob_in, ob_ref))
    vectors += ((mg_in, mg_ref), (ms_in, ms_ref), (ub_in, ub_ref), (db_in, db_ref))
    vector_copies = [pltpu.make_async_copy(a, b.at[0], vec_sem.at[v]) for v, (a, b) in enumerate(vectors)]
    token_copy = pltpu.make_async_copy(tok_in, tok_ref, io_sem.at[0])
    token_copy.start()
    for copy in vector_copies:
        copy.start()

    barrier = pltpu.get_barrier_semaphore()
    for t in range(n):
        if t:
            pl.semaphore_signal(barrier, inc=1, device_id=(d, (s + t) % n), device_id_type=MESH)
        pl.semaphore_signal(barrier, inc=1, device_id=(sibling, (s + t) % n), device_id_type=MESH)
    for j in range(1, pairs):
        for cc in range(2):
            there = (pair + j) % pairs * 2 + cc
            pl.semaphore_signal(barrier, inc=1, device_id=(there, s), device_id_type=MESH)
    pl.semaphore_wait(barrier, 2 * n - 1 + 2 * (pairs - 1))

    def remote(src, dst, send, recv, device):
        return pltpu.make_async_remote_copy(
            src_ref=src, dst_ref=dst, send_sem=send, recv_sem=recv, device_id=device, device_id_type=MESH
        )

    chunks = tok // NORM_ROWS

    def rows_at(c):
        return pl.ds(c * NORM_ROWS, NORM_ROWS)

    def token_z(i, c):
        there = core * images + i
        return remote(
            tok_ref.at[i, rows_at(c)],
            xin.at[s, rows_at(c)],
            t_send.at[i, c],
            t_recv.at[z, c],
            (d, there * across + y),
        )

    def token_z_in(zp, c):
        slot = xin.at[zp * across + y, rows_at(c)]
        return remote(slot, slot, t_send.at[0, c], t_recv.at[zp, c], (d, s))

    def token_y(zp, dy, c, src=None):
        there = z * across + (y + dy) % across
        slot = xin.at[zp * across + y, rows_at(c)]
        return remote(
            slot if src is None else src, slot, ty_send.at[zp, dy, c], ty_recv.at[zp, dy, c], (d, there)
        )

    def side_slot(zp, dy):
        return zp * across + (y + across - dy) % across

    def token_y_in(zp, dy, c):
        slot = xin.at[side_slot(zp, dy), rows_at(c)]
        return remote(slot, slot, ty_send.at[zp, dy, c], ty_recv.at[zp, dy, c], (d, s))

    def token_s(sp, c, src=None):
        slot = xin.at[sp, rows_at(c)]
        return remote(slot if src is None else src, slot, ts_send.at[sp, c], ts_recv.at[sp, c], (sibling, s))

    def own_tokens(c):
        return tok_ref.at[z % images, rows_at(c)]

    def q_first(group):
        return pl.multiple_of(
            group * plan.columns // LANES * LANES - group // (2 * across - 1) * plan.shift_back, LANES
        )

    def q_columns(part, group):
        low, high = plan.cuts[part], plan.cuts[part + 1]
        return pl.ds(pl.multiple_of(q_first(group) + low, LANES), high - low)

    def q_part(part):
        return pl.ds(plan.cuts[part], plan.cuts[part + 1] - plan.cuts[part])

    q_half = plan.q_rows // 2

    def q_slab(owner, half):
        return pl.ds(pl.multiple_of(owner * plan.q_rows + half * q_half, 8), q_half)

    def q_x(part, j, cc):
        half = z % 2
        return remote(
            wq_ref.at[pl.ds(pl.multiple_of(half * q_half, 8), q_half), q_columns(part, 2 * y + cc)],
            wraw.at[q_slab(d, half), q_part(part)],
            q_send.at[part, j, cc],
            q_recv.at[part, j, core],
            ((pair + j) % pairs * 2 + cc, s),
        )

    def q_x_in(part, j, cc):
        slot = wraw.at[q_slab((pair + pairs - j) % pairs * 2 + cc, z % 2), q_part(part)]
        return remote(slot, slot, q_send.at[part, j, cc], q_recv.at[part, j, cc], (d, s))

    def q_z(part, j, cc, arriving=False):
        half = 1 - z % 2 if arriving else z % 2
        slot = wraw.at[q_slab((pair + pairs - j) % pairs * 2 + cc, half), q_part(part)]
        there = z_near * across + y
        return remote(slot, slot, qz_send.at[part, j, cc], qz_recv.at[part, j, cc], (d, there))

    def q_full(owner):
        return pl.ds(pl.multiple_of(owner * plan.q_rows, 16), plan.q_rows)

    def q_s(part, arriving=False):
        return remote(
            wq_ref.at[:, q_columns(part, 2 * y + 1 - core)],
            wraw.at[q_full(sibling if arriving else d), q_part(part)],
            qs_send.at[part],
            qs_recv.at[part],
            (sibling, s),
        )

    def q_mine(part):
        return pltpu.make_async_copy(
            wq_ref.at[:, q_columns(part, 2 * y + core)], wraw.at[q_full(d), q_part(part)], q_own.at[part]
        )

    def slab(k, owner):
        depth = shards_of[k].shape[0]
        return pl.ds(pl.multiple_of(owner * depth, 16), depth)

    def piece_columns(piece, other=False):
        k, low, columns, along_z = piece
        half = z % 2 if along_z else y % 2
        if other:
            half = 1 - half
        return pl.ds(pl.multiple_of(half * (wholes[k].shape[1] // 2) + low, LANES), columns)

    def owner_of(j):
        return (pair + pairs - j) % pairs * 2 + core

    def w_x(q, j, arriving=False):
        k = pieces[q][0]
        columns = piece_columns(pieces[q])
        return remote(
            shards_of[k].at[:, columns],
            wholes[k].at[slab(k, owner_of(j) if arriving else d), columns],
            x_send.at[q, j],
            x_recv.at[q, j],
            ((pair + j) % pairs * 2 + core, s),
        )

    def w_p(q, j, arriving=False):
        k, along_z = pieces[q][0], pieces[q][3]
        slot = wholes[k].at[slab(k, owner_of(j)), piece_columns(pieces[q], arriving)]
        there = z_near * across + y if along_z else z * across + y_near
        return remote(slot, slot, p_send.at[q, j], p_recv.at[q, j], (d, there))

    def w_s(q, j, second, arriving=False):
        k = pieces[q][0]
        owner = (pair + pairs - j) % pairs * 2 + (1 - core if arriving else core)
        slot = wholes[k].at[slab(k, owner), piece_columns(pieces[q], second)]
        way = 1 if second else 0
        return remote(slot, slot, s_send.at[q, j, way], s_recv.at[q, j, way], (sibling, s))

    def w_so(k, arriving=False):
        return remote(
            shards_of[k],
            wholes[k].at[slab(k, sibling if arriving else d)],
            so_send.at[k],
            so_recv.at[k],
            (sibling, s),
        )

    def w_own(k):
        return pltpu.make_async_copy(shards_of[k], wholes[k].at[slab(k, d)], own_sem.at[k])

    def pass_first(q):
        for j in range(1, pairs):
            w_x(q, j, True).wait_recv()
            w_p(q, j).start()
            w_s(q, j, False).start()

    def pass_second(q):
        for j in range(1, pairs):
            w_p(q, j, True).wait_recv()
            w_s(q, j, True).start()

    def arrived(k):
        w_own(k).wait()
        w_so(k, True).wait_recv()
        for q, piece in enumerate(pieces):
            if piece[0] == k:
                for j in range(1, pairs):
                    for second in (False, True):
                        w_s(q, j, second, True).wait_recv()

    def ctx_copy(part, sp, group, slot):
        low, high = plan.sends[part]
        return remote(
            mixed.at[sp, :, pl.ds(low, high - low)],
            landed.at[group, slot, :, pl.ds(low, high - low)],
            c_send.at[part, sp],
            c_recv.at[part, group, slot],
            (pair * 2 + z // images, sp),
        )

    def sends_in(part):
        return plan.sends[part][0] < plan.sends[part][1]

    token_copy.wait()
    for c in range(chunks):
        for k in range(images):
            i = (1 - core) * k + core * (images - 1 - k)

            @pl.when(core * images + i != z)
            def _():
                token_z(i, c).start()

        @pl.when(mine)
        def _():
            for dy in range(1, across):
                token_y(z, dy, c, own_tokens(c)).start()
            token_s(s, c, own_tokens(c)).start()

    def q_start(part):
        for j in range(1, pairs):
            q_x(part, j, 0).start()
            q_x(part, j, 1).start()

    def w_start(q):
        for j in range(1, pairs):
            w_x(q, j).start()

    q_start(0)
    w_start(0)
    for part in range(1, n_parts):
        q_start(part)
    for part in range(n_parts):
        q_mine(part).start()
        q_s(part).start()
    for q in range(1, len(pieces)):
        w_start(q)

    wbuf[...] = jnp.zeros_like(wbuf)
    for copy in vector_copies:
        copy.wait()
    group = 2 * y + core
    per_part = plan.part_heads * 3
    for rest in sorted(set(plan.rests)):
        which = [g for g, r in enumerate(plan.rests) if r == rest]
        hit = group == which[0]
        for g in which[1:]:
            hit = jnp.logical_or(hit, group == g)

        @pl.when(hit)
        def _(rest=rest):
            row = qb_ref[:, pl.ds(q_first(group), plan.window)]
            for g in range(2 * per_part):
                piece = row[:, rest + g * HEAD_DIM : rest + (g + 1) * HEAD_DIM]
                at = g % per_part * LANES
                ones = jnp.full((1, LANES - HEAD_DIM), 1.0 if g % 3 == 2 else 0.0, jnp.float32)
                bpad[g // per_part, :, at : at + LANES] = jnp.concatenate([piece, ones], axis=-1)

    pair_rows = 2 * plan.q_rows

    def pad_weights(part, j):
        rows = pl.ds(pl.multiple_of((pair + j) % pairs * pair_rows, 16), pair_rows)
        for rest in sorted(set(plan.rests)):
            which = [g for g, r in enumerate(plan.rests) if r == rest]
            hit = group == which[0]
            for g in which[1:]:
                hit = jnp.logical_or(hit, group == g)

            @pl.when(hit)
            def _(rest=rest):
                for g in range(per_part):
                    low = rest + (part * per_part + g) * HEAD_DIM
                    wbuf[part, rows, g * LANES : g * LANES + HEAD_DIM] = wraw[rows, low : low + HEAD_DIM]

    def pad_others(part):
        for j in range(1, pairs):
            for cc in range(2):
                q_z(part, j, cc, True).wait_recv()
        for j in range(1, pairs):
            pad_weights(part, j)

    def pad_own():
        for part in range(n_parts):
            q_mine(part).wait()
            q_s(part, True).wait_recv()
        for part in range(2):
            pad_weights(part, 0)

    def norm_chunk(slot, c):
        at = pl.ds(pl.multiple_of(slot * tok + c * NORM_ROWS, 16), NORM_ROWS)
        block = xin[slot, rows_at(c), :].astype(jnp.float32)
        xn[at, :] = normalize(block, pg_ref[...], ps_ref[...]).astype(HALF)

    def side(zp, c):
        @pl.when(mine)
        def _():
            for dy in range(1, across):
                token_y_in(zp, dy, c).wait_recv()
                token_s(side_slot(zp, dy), c).start()

        @pl.when(others)
        def _():
            for dy in range(1, across):
                token_s(side_slot(zp, dy), c).wait_recv()

    def norm_side(zp, c):
        for dy in range(1, across):
            norm_chunk(side_slot(zp, dy), c)

    def far(zp, c):
        slot = zp * across + y

        @pl.when(mine)
        def _():
            token_z_in(zp, c).wait_recv()
            for dy in range(1, across):
                token_y(zp, dy, c).start()
            token_s(slot, c).start()

        @pl.when(others)
        def _():
            token_s(slot, c).wait_recv()

    def q_relay(part):
        for j in range(1, pairs):
            for cc in range(2):
                q_x_in(part, j, cc).wait_recv()
                q_z(part, j, cc).start()

    @pl.when(mine)
    def _():
        xin[s] = tok_ref[z % images]

    @pl.when(others)
    def _():
        for c in range(chunks):
            token_s(s, c).wait_recv()

    for c in range(chunks):
        norm_chunk(s, c)
    for c in range(chunks):
        side(z, c)
        norm_side(z, c)
    pad_own()
    for c in range(chunks):
        for zp in z_order[1:]:
            far(zp, c)
        if c == 0:
            q_relay(0)
        if c:
            for zp in z_order[1:]:
                side(zp, c - 1)
        for zp in z_order[1:]:
            norm_chunk(zp * across + y, c)
            if c:
                norm_side(zp, c - 1)
    pass_first(0)
    for zp in z_order[1:]:
        side(zp, chunks - 1)
        norm_side(zp, chunks - 1)

    for k in range(3):
        w_own(k).start()
        w_so(k).start()

    block_rows = across * tok

    def project(part):
        def one(i, carry):
            at = pl.ds(pl.multiple_of(i * block_rows, 16), block_rows)
            result = jnp.dot(xn[at, :], wbuf[part], preferred_element_type=jnp.float32) + bpad[part]
            packed[part, at, :] = result.astype(HALF)
            return carry

        lax.fori_loop(0, groups, one, 0)

    def attend(part, after):
        def one(step, carry):
            near = (step + 1) // 2 % 2
            far = 1 - step // 2
            zp = (z + near * (1 - 2 * (z % 2)) + 2 * far) % groups
            at = pl.ds(pl.multiple_of(zp * block_rows, 16), block_rows)
            outs = []
            for h in range(plan.part_heads):
                base = h * 3 * LANES
                queries = packed[part, at, base : base + LANES]
                key_rows = packed[part, :, base + LANES : base + 2 * LANES]
                value_rows = packed[part, :, base + 2 * LANES : base + 3 * LANES]
                scores = lax.dot_general(
                    queries, key_rows, (((1,), (1,)), ((), ())), preferred_element_type=jnp.float32
                )
                highest = jnp.max(scores, axis=-1, keepdims=True)
                weights = jnp.exp2((scores - highest) * factor).astype(HALF)
                summed = jnp.dot(weights, value_rows, preferred_element_type=jnp.float32)
                outs.append(summed[:, :HEAD_DIM] / summed[:, HEAD_DIM : HEAD_DIM + 1])
            whole = (jnp.concatenate(outs, axis=-1) if len(outs) > 1 else outs[0]).astype(HALF)
            for yy in range(across):
                sp = zp * across + yy
                here = slice(part * plan.span, (part + 1) * plan.span)
                mixed[sp, :, here] = whole[yy * tok : (yy + 1) * tok]
                own = jnp.logical_and(mine, sp == s)

                @pl.when(own)
                def _():
                    landed[group, z % images, :, here] = whole[yy * tok : (yy + 1) * tok]

                if sends_in(part):

                    @pl.when(jnp.logical_not(own))
                    def _():
                        ctx_copy(part, sp, group, z % images).start()

            for when, action in after:

                @pl.when(step == when)
                def _():
                    action()

            return carry

        lax.fori_loop(0, groups, one, 0)

    pad_others(0)
    project(0)
    for part in range(1, n_parts):
        q_relay(part)
    attend(0, [])
    pass_first(1)
    pad_others(1)
    project(1)
    attend(1, [])
    pass_first(2)
    pass_first(3)
    pass_first(4)

    def context_in(part, gg, i):
        if not sends_in(part):
            return
        yy, cc = gg // 2, gg % 2
        source = (core * images + i) * across + yy
        own = jnp.logical_and(source == s, core == cc)
        low, high = plan.sends[part]
        slot = landed.at[gg, i, :, pl.ds(low, high - low)]

        @pl.when(jnp.logical_not(own))
        def _():
            remote(
                slot, slot, c_send.at[part, 0], c_recv.at[part, gg, i], (pair * 2 + cc, source)
            ).wait_recv()

    def contexts_in(part):
        for i in range(images):
            for gg in range(2 * across):
                context_in(part, gg, i)

    def gather_contexts():
        columns = plan.heads * HEAD_DIM
        for i in range(images):
            for gg in range(2 * across):
                ctx[i * tok : (i + 1) * tok, gg * columns : (gg + 1) * columns] = landed[gg, i]

    contexts_in(0)
    pass_second(0)
    pass_second(1)
    pass_first(5)
    contexts_in(1)
    gather_contexts()
    arrived(0)
    row_count = images * tok

    def tile_of(c):
        return pl.ds(pl.multiple_of(c * 2 * LANES, 2 * LANES), 2 * LANES)

    def out_tile(c, carry):
        cols = tile_of(c)
        attended = jnp.dot(ctx[...], w_out[:, cols], preferred_element_type=jnp.float32)
        residual = tok_ref[:, :, cols].astype(jnp.float32).reshape(row_count, 2 * LANES)
        mid[:, cols] = residual + attended + ob_ref[:, cols]
        return carry

    lax.fori_loop(0, plan.width // (2 * LANES), out_tile, 0)

    def second_norm(i, carry):
        at = pl.ds(pl.multiple_of(i * NORM_ROWS, 16), NORM_ROWS)
        ctx[at, :] = normalize(mid[at, :], mg_ref[...], ms_ref[...]).astype(HALF)
        return carry

    lax.fori_loop(0, row_count // NORM_ROWS, second_norm, 0)

    def lift(cols):
        lifted = jnp.dot(ctx[...], w_up[:, cols], preferred_element_type=jnp.float32)
        lifted = lifted + ub_ref[:, cols]
        hid[:, cols] = (0.5 * lifted * (1.0 + lax.erf(lifted * math.sqrt(0.5)))).astype(HALF)

    def piece_in(q, second):
        for j in range(1, pairs):
            w_s(q, j, second, True).wait_recv()

    ups = [q for q, piece in enumerate(pieces) if piece[0] == 1]
    downs = [q for q, piece in enumerate(pieces) if piece[0] == 2]
    w_own(1).wait()
    w_so(1, True).wait_recv()
    for q in ups:
        piece_in(q, False)
        lift(piece_columns(pieces[q], False))
    pass_first(6)
    for p, q in enumerate(ups[1:]):
        pass_second(q)
        before = ups[p]
        piece_in(before, True)
        lift(piece_columns(pieces[before], True))
    pass_first(7)
    piece_in(ups[-1], True)
    lift(piece_columns(pieces[ups[-1]], True))

    def result_copy(slot, cols):
        return pltpu.make_async_copy(o_ref.at[:, :, cols], o_out.at[:, :, cols], io_sem.at[slot + 1])

    def lower(slot, cols):
        lowered = jnp.dot(hid[...], w_down[:, cols], preferred_element_type=jnp.float32)
        result = (mid[:, cols] + lowered + db_ref[:, cols]).astype(HALF)
        o_ref[:, :, cols] = result.reshape(images, tok, cols.size)
        result_copy(slot, cols).start()

    w_own(2).wait()
    w_so(2, True).wait_recv()
    for p, q in enumerate(downs):
        piece_in(q, False)
        lower(2 * q, piece_columns(pieces[q], False))
        pass_second(q)
    for q in downs:
        piece_in(q, True)
        lower(2 * q + 1, piece_columns(pieces[q], True))
    for second in (False, True):
        for q in downs:
            result_copy(2 * q + second, piece_columns(pieces[q], second)).wait()

    for c in range(chunks):
        for k in range(images):

            @pl.when(core * images + k != z)
            def _():
                token_z(k, c).wait_send()

        @pl.when(mine)
        def _():
            for zp in range(groups):
                for dy in range(1, across):
                    token_y(zp, dy, c).wait_send()
            for sp in range(n):
                token_s(sp, c).wait_send()

    for part in range(n_parts):
        q_s(part).wait_send()
        for j in range(1, pairs):
            for cc in range(2):
                q_x(part, j, cc).wait_send()
                q_z(part, j, cc).wait_send()
    for k in range(3):
        w_so(k).wait_send()
    for q in range(len(pieces)):
        for j in range(1, pairs):
            w_x(q, j).wait_send()
            w_p(q, j).wait_send()
            w_s(q, j, False).wait_send()
            w_s(q, j, True).wait_send()
    for part in range(2):
        for sp in range(n):

            @pl.when(jnp.logical_not(jnp.logical_and(mine, sp == s)))
            def _():
                if sends_in(part):
                    ctx_copy(part, sp, group, z % images).wait_send()


def shards(n, n_dp, tokens, pre_gain, pre_shift, w_qkv, qkv_bias, w_out, out_bias, mlp_gain, mlp_shift,
           w_up, up_bias, w_down, down_bias):
    images, tok, width = tokens.shape
    hidden = w_up.shape[1]
    plan = Plan(n, n_dp, images, tok, width, hidden, w_qkv.shape[1])
    rows = images * tok
    dma = pltpu.SemaphoreType.DMA
    anywhere = pl.BlockSpec(memory_space=pl.ANY)
    pairs, groups, across = plan.pairs, plan.groups, plan.across
    n_pieces = len(pieces_of(plan))
    parts = len(plan.cuts) - 1
    chunks = tok // NORM_ROWS
    vectors = (pre_gain, pre_shift, qkv_bias, out_bias, mlp_gain, mlp_shift, up_bias, down_bias)
    return pl.pallas_call(
        functools.partial(layer_kernel, plan),
        out_shape=jax.ShapeDtypeStruct(tokens.shape, HALF),
        in_specs=[anywhere] * 13,
        out_specs=anywhere,
        scratch_shapes=[
            pltpu.VMEM(tokens.shape, HALF),
            pltpu.VMEM(tokens.shape, HALF),
            dma((1 + 2 * n_pieces,)),
            *[pltpu.VMEM((1, v.shape[0]), jnp.float32) for v in vectors],
            dma((8,)),
            pltpu.VMEM((n, tok, width), HALF),
            pltpu.VMEM((plan.length, width), HALF),
            pltpu.VMEM((width, plan.window), HALF),
            pltpu.VMEM((2, width, plan.part_columns), HALF),
            pltpu.VMEM((2, 1, plan.part_columns), jnp.float32),
            pltpu.VMEM((2, plan.length, plan.part_columns), HALF),
            pltpu.VMEM((n, tok, 2 * plan.span), HALF),
            pltpu.VMEM((2 * across, images, tok, 2 * plan.span), HALF),
            pltpu.VMEM((rows, width), HALF),
            pltpu.VMEM((rows, width), jnp.float32),
            pltpu.VMEM((rows, hidden), HALF),
            pltpu.VMEM((width, width), HALF),
            pltpu.VMEM((width, hidden), HALF),
            pltpu.VMEM((hidden, width), HALF),
            dma((images, chunks)),
            dma((groups, chunks)),
            dma((groups, across, chunks)),
            dma((groups, across, chunks)),
            dma((n, chunks)),
            dma((n, chunks)),
            dma((parts, pairs, 2)),
            dma((parts, pairs, 2)),
            dma((parts, pairs, 2)),
            dma((parts, pairs, 2)),
            dma((parts,)),
            dma((parts,)),
            dma((parts,)),
            dma((n_pieces, pairs)),
            dma((n_pieces, pairs)),
            dma((n_pieces, pairs)),
            dma((n_pieces, pairs)),
            dma((n_pieces, pairs, 2)),
            dma((n_pieces, pairs, 2)),
            dma((3,)),
            dma((3,)),
            dma((3,)),
            dma((2, n)),
            dma((2, 2 * across, images)),
        ],
        compiler_params=pltpu.CompilerParams(
            collective_id=0, has_side_effects=True, vmem_limit_bytes=67043328
        ),
        name="encoder_layer",
    )(
        tokens,
        w_qkv,
        w_out,
        w_up,
        w_down,
        *vectors,
    )


def solution(mesh):
    in_specs = (
        P("dp", "seq", None),
        P(),
        P(),
        P("dp", None),
        P(),
        P("dp", None),
        P(),
        P(),
        P(),
        P("dp", None),
        P(),
        P("dp", None),
        P(),
    )
    out_specs = P("dp", "seq", None)
    step = functools.partial(shards, mesh.shape["seq"], mesh.shape["dp"])
    return jax.shard_map(step, mesh=mesh, in_specs=in_specs, out_specs=out_specs, check_vma=False)
```

```python
import functools
import math

import jax
import jax.numpy as jnp
from jax import lax
from jax.experimental import pallas as pl
from jax.experimental.pallas import tpu as pltpu
from jax.sharding import PartitionSpec as P

HEADS = 16
HEAD_DIM = 80
LANES = 128
EPSILON = 1e-05
MESH = pl.DeviceIdType.MESH
HALF = jnp.bfloat16
NORM_ROWS = 48


def up_to(value, step):
    return -(-value // step) * step


class Plan:
    def __init__(self, n, n_dp, images, tok, width, hidden, qkv_width):
        self.n, self.n_dp, self.images, self.tok = n, n_dp, images, tok
        self.width, self.hidden, self.qkv_width = width, hidden, qkv_width
        self.pairs = n_dp // 2
        self.groups = 2 * images
        self.across = n // self.groups
        self.heads = HEADS // (2 * self.across)
        self.length = n * tok
        self.part_heads = self.heads // 2
        self.span = self.part_heads * HEAD_DIM
        total = 2 * self.span
        self.full = total // LANES
        self.rest = total % LANES
        self.fold = 2 if self.rest == LANES // 2 and tok % 16 == 0 else 1
        rest_rows = tok // self.fold if self.rest else 0
        self.ctx_rows = self.full * tok + rest_rows
        early = self.span // LANES * tok
        self.sends = ((0, early), (early, self.ctx_rows))
        self.part_columns = self.part_heads * 3 * LANES
        columns = self.heads * 3 * HEAD_DIM
        starts = [g * columns for g in range(2 * self.across)]
        rest = max(start % LANES for start in starts)
        self.window = up_to(rest + columns, LANES)
        last = starts[-1] // LANES * LANES
        self.shift_back = max(0, last + self.window - qkv_width)
        firsts = [start // LANES * LANES for start in starts]
        firsts[-1] -= self.shift_back
        self.rests = [start - first for start, first in zip(starts, firsts)]
        self.columns = columns
        cut = min(self.window, up_to(max(self.rests) + columns // 2, LANES))
        self.cuts = (0, cut, self.window) if cut < self.window else (0, cut)
        self.q_rows = width // n_dp


def normalize(features, gain, shift):
    average = jnp.mean(features, axis=-1, keepdims=True)
    centered = features - average
    spread = jnp.mean(centered * centered, axis=-1, keepdims=True)
    return centered * lax.rsqrt(spread + EPSILON) * gain + shift


def thirds(columns, parts):
    tiles = columns // LANES
    sizes = [(tiles + parts - 1 - p) // parts * LANES for p in range(parts)]
    return [(sum(sizes[:p]), size) for p, size in enumerate(sizes) if size]


def pieces_of(plan):
    cuts = (thirds(plan.width // 2, 1), thirds(plan.hidden // 2, 4), thirds(plan.width // 2, 3))
    along = ((0,), (0, 0, 0, 1), (1, 0, 1))
    return tuple((k, low, size, along[k][p]) for k in range(3) for p, (low, size) in enumerate(cuts[k]))


def layer_kernel(
    plan,
    tok_in,
    wq_ref,
    wo_ref,
    wu_ref,
    wd_ref,
    pg_in,
    ps_in,
    qb_in,
    ob_in,
    mg_in,
    ms_in,
    ub_in,
    db_in,
    o_out,
    tok_ref,
    o_ref,
    io_sem,
    pg_ref,
    ps_ref,
    qb_ref,
    ob_ref,
    mg_ref,
    ms_ref,
    ub_ref,
    db_ref,
    vec_sem,
    xin,
    xn,
    wraw,
    wbuf,
    bpad,
    packed,
    kept,
    mixed,
    landed,
    ctx,
    mid,
    hid,
    w_out,
    w_up,
    w_down,
    t_send,
    t_recv,
    ty_send,
    ty_recv,
    ts_send,
    ts_recv,
    q_send,
    q_recv,
    qz_send,
    qz_recv,
    qs_send,
    qs_recv,
    q_own,
    x_send,
    x_recv,
    p_send,
    p_recv,
    s_send,
    s_recv,
    so_send,
    so_recv,
    own_sem,
    c_send,
    c_recv,
):
    n, n_dp, images, tok = plan.n, plan.n_dp, plan.images, plan.tok
    groups, across, pairs = plan.groups, plan.across, plan.pairs
    d, s = lax.axis_index("dp"), lax.axis_index("seq")
    core = d % 2
    pair = d // 2
    sibling = d + 1 - 2 * core
    z, y = s // across, s % across
    z_near = z + 1 - 2 * (z % 2)
    y_near = y + 1 - 2 * (y % 2)
    z_order = (z, z_near, (z + 2) % groups, (z_near + 2) % groups)
    mine = z // images == core
    others = z // images != core
    shards_of = (wo_ref, wu_ref, wd_ref)
    wholes = (w_out, w_up, w_down)
    pieces = pieces_of(plan)
    n_parts = len(plan.cuts) - 1
    factor = math.log2(math.e) / math.sqrt(HEAD_DIM)

    vectors = ((pg_in, pg_ref), (ps_in, ps_ref), (qb_in, qb_ref), (ob_in, ob_ref))
    vectors += ((mg_in, mg_ref), (ms_in, ms_ref), (ub_in, ub_ref), (db_in, db_ref))
    vector_copies = [pltpu.make_async_copy(a, b.at[0], vec_sem.at[v]) for v, (a, b) in enumerate(vectors)]
    token_copy = pltpu.make_async_copy(tok_in, tok_ref, io_sem.at[0])
    token_copy.start()
    for copy in vector_copies:
        copy.start()

    barrier = pltpu.get_barrier_semaphore()
    for t in range(n):
        if t:
            pl.semaphore_signal(barrier, inc=1, device_id=(d, (s + t) % n), device_id_type=MESH)
        pl.semaphore_signal(barrier, inc=1, device_id=(sibling, (s + t) % n), device_id_type=MESH)
    for j in range(1, pairs):
        for cc in range(2):
            there = (pair + j) % pairs * 2 + cc
            pl.semaphore_signal(barrier, inc=1, device_id=(there, s), device_id_type=MESH)
    pl.semaphore_wait(barrier, 2 * n - 1 + 2 * (pairs - 1))

    def remote(src, dst, send, recv, device):
        return pltpu.make_async_remote_copy(
            src_ref=src, dst_ref=dst, send_sem=send, recv_sem=recv, device_id=device, device_id_type=MESH
        )

    chunks = tok // NORM_ROWS

    def rows_at(c):
        return pl.ds(c * NORM_ROWS, NORM_ROWS)

    def token_z(i, c):
        there = core * images + i
        return remote(
            tok_ref.at[i, rows_at(c)],
            xin.at[s, rows_at(c)],
            t_send.at[i, c],
            t_recv.at[z, c],
            (d, there * across + y),
        )

    def token_z_in(zp, c):
        slot = xin.at[zp * across + y, rows_at(c)]
        return remote(slot, slot, t_send.at[0, c], t_recv.at[zp, c], (d, s))

    def token_y(zp, dy, c, src=None):
        there = z * across + (y + dy) % across
        slot = xin.at[zp * across + y, rows_at(c)]
        return remote(
            slot if src is None else src, slot, ty_send.at[zp, dy, c], ty_recv.at[zp, dy, c], (d, there)
        )

    def side_slot(zp, dy):
        return zp * across + (y + across - dy) % across

    def token_y_in(zp, dy, c):
        slot = xin.at[side_slot(zp, dy), rows_at(c)]
        return remote(slot, slot, ty_send.at[zp, dy, c], ty_recv.at[zp, dy, c], (d, s))

    def token_s(sp, c, src=None):
        slot = xin.at[sp, rows_at(c)]
        return remote(slot if src is None else src, slot, ts_send.at[sp, c], ts_recv.at[sp, c], (sibling, s))

    def own_tokens(c):
        return tok_ref.at[z % images, rows_at(c)]

    def q_first(group):
        return pl.multiple_of(
            group * plan.columns // LANES * LANES - group // (2 * across - 1) * plan.shift_back, LANES
        )

    def q_columns(part, group):
        low, high = plan.cuts[part], plan.cuts[part + 1]
        return pl.ds(pl.multiple_of(q_first(group) + low, LANES), high - low)

    def q_part(part):
        return pl.ds(plan.cuts[part], plan.cuts[part + 1] - plan.cuts[part])

    q_half = plan.q_rows // 2

    def q_slab(owner, half):
        return pl.ds(pl.multiple_of(owner * plan.q_rows + half * q_half, 8), q_half)

    def q_x(part, j, cc):
        half = z % 2
        return remote(
            wq_ref.at[pl.ds(pl.multiple_of(half * q_half, 8), q_half), q_columns(part, 2 * y + cc)],
            wraw.at[q_slab(d, half), q_part(part)],
            q_send.at[part, j, cc],
            q_recv.at[part, j, core],
            ((pair + j) % pairs * 2 + cc, s),
        )

    def q_x_in(part, j, cc):
        slot = wraw.at[q_slab((pair + pairs - j) % pairs * 2 + cc, z % 2), q_part(part)]
        return remote(slot, slot, q_send.at[part, j, cc], q_recv.at[part, j, cc], (d, s))

    def q_z(part, j, cc, arriving=False):
        half = 1 - z % 2 if arriving else z % 2
        slot = wraw.at[q_slab((pair + pairs - j) % pairs * 2 + cc, half), q_part(part)]
        there = z_near * across + y
        return remote(slot, slot, qz_send.at[part, j, cc], qz_recv.at[part, j, cc], (d, there))

    def q_full(owner):
        return pl.ds(pl.multiple_of(owner * plan.q_rows, 16), plan.q_rows)

    def q_s(part, arriving=False):
        return remote(
            wq_ref.at[:, q_columns(part, 2 * y + 1 - core)],
            wraw.at[q_full(sibling if arriving else d), q_part(part)],
            qs_send.at[part],
            qs_recv.at[part],
            (sibling, s),
        )

    def q_mine(part):
        return pltpu.make_async_copy(
            wq_ref.at[:, q_columns(part, 2 * y + core)], wraw.at[q_full(d), q_part(part)], q_own.at[part]
        )

    def slab(k, owner):
        depth = shards_of[k].shape[0]
        return pl.ds(pl.multiple_of(owner * depth, 16), depth)

    def piece_columns(piece, other=False):
        k, low, columns, along_z = piece
        half = z % 2 if along_z else y % 2
        if other:
            half = 1 - half
        return pl.ds(pl.multiple_of(half * (wholes[k].shape[1] // 2) + low, LANES), columns)

    def owner_of(j):
        return (pair + pairs - j) % pairs * 2 + core

    def w_x(q, j, arriving=False):
        k = pieces[q][0]
        columns = piece_columns(pieces[q])
        return remote(
            shards_of[k].at[:, columns],
            wholes[k].at[slab(k, owner_of(j) if arriving else d), columns],
            x_send.at[q, j],
            x_recv.at[q, j],
            ((pair + j) % pairs * 2 + core, s),
        )

    def w_p(q, j, arriving=False):
        k, along_z = pieces[q][0], pieces[q][3]
        slot = wholes[k].at[slab(k, owner_of(j)), piece_columns(pieces[q], arriving)]
        there = z_near * across + y if along_z else z * across + y_near
        return remote(slot, slot, p_send.at[q, j], p_recv.at[q, j], (d, there))

    def w_s(q, j, second, arriving=False):
        k = pieces[q][0]
        owner = (pair + pairs - j) % pairs * 2 + (1 - core if arriving else core)
        slot = wholes[k].at[slab(k, owner), piece_columns(pieces[q], second)]
        way = 1 if second else 0
        return remote(slot, slot, s_send.at[q, j, way], s_recv.at[q, j, way], (sibling, s))

    def w_so(k, arriving=False):
        return remote(
            shards_of[k],
            wholes[k].at[slab(k, sibling if arriving else d)],
            so_send.at[k],
            so_recv.at[k],
            (sibling, s),
        )

    def w_own(k):
        return pltpu.make_async_copy(shards_of[k], wholes[k].at[slab(k, d)], own_sem.at[k])

    def pass_first(q):
        for j in range(1, pairs):
            w_x(q, j, True).wait_recv()
            w_p(q, j).start()
            w_s(q, j, False).start()

    def pass_second(q):
        for j in range(1, pairs):
            w_p(q, j, True).wait_recv()
            w_s(q, j, True).start()

    def arrived(k):
        w_own(k).wait()
        w_so(k, True).wait_recv()
        for q, piece in enumerate(pieces):
            if piece[0] == k:
                for j in range(1, pairs):
                    for second in (False, True):
                        w_s(q, j, second, True).wait_recv()

    def ctx_copy(part, sp, group, slot):
        low, high = plan.sends[part]
        return remote(
            mixed.at[sp, pl.ds(low, high - low)],
            landed.at[group, slot, pl.ds(low, high - low)],
            c_send.at[part, sp],
            c_recv.at[part, group, slot],
            (pair * 2 + z // images, sp),
        )

    def sends_in(part):
        return plan.sends[part][0] < plan.sends[part][1]

    token_copy.wait()
    for c in range(chunks):
        for k in range(images):
            i = (1 - core) * k + core * (images - 1 - k)

            @pl.when(core * images + i != z)
            def _():
                token_z(i, c).start()

        @pl.when(mine)
        def _():
            for dy in range(1, across):
                token_y(z, dy, c, own_tokens(c)).start()
            token_s(s, c, own_tokens(c)).start()

    def q_start(part):
        for j in range(1, pairs):
            q_x(part, j, 0).start()
            q_x(part, j, 1).start()

    def w_start(q):
        for j in range(1, pairs):
            w_x(q, j).start()

    q_start(0)
    w_start(0)
    for part in range(1, n_parts):
        q_start(part)
    for part in range(n_parts):
        q_mine(part).start()
        q_s(part).start()
    for q in range(1, len(pieces)):
        w_start(q)

    wbuf[...] = jnp.zeros_like(wbuf)
    for copy in vector_copies:
        copy.wait()
    group = 2 * y + core
    per_part = plan.part_heads * 3
    for rest in sorted(set(plan.rests)):
        which = [g for g, r in enumerate(plan.rests) if r == rest]
        hit = group == which[0]
        for g in which[1:]:
            hit = jnp.logical_or(hit, group == g)

        @pl.when(hit)
        def _(rest=rest):
            row = qb_ref[:, pl.ds(q_first(group), plan.window)]
            for g in range(2 * per_part):
                piece = row[:, rest + g * HEAD_DIM : rest + (g + 1) * HEAD_DIM]
                at = g % per_part * LANES
                ones = jnp.full((1, LANES - HEAD_DIM), 1.0 if g % 3 == 2 else 0.0, jnp.float32)
                bpad[g // per_part, :, at : at + LANES] = jnp.concatenate([piece, ones], axis=-1)

    pair_rows = 2 * plan.q_rows

    def pad_weights(part, j):
        rows = pl.ds(pl.multiple_of((pair + j) % pairs * pair_rows, 16), pair_rows)
        for rest in sorted(set(plan.rests)):
            which = [g for g, r in enumerate(plan.rests) if r == rest]
            hit = group == which[0]
            for g in which[1:]:
                hit = jnp.logical_or(hit, group == g)

            @pl.when(hit)
            def _(rest=rest):
                for g in range(per_part):
                    low = rest + (part * per_part + g) * HEAD_DIM
                    wbuf[part, rows, g * LANES : g * LANES + HEAD_DIM] = wraw[rows, low : low + HEAD_DIM]

    def pad_others(part):
        for j in range(1, pairs):
            for cc in range(2):
                q_z(part, j, cc, True).wait_recv()
        for j in range(1, pairs):
            pad_weights(part, j)

    def pad_own():
        for part in range(n_parts):
            q_mine(part).wait()
            q_s(part, True).wait_recv()
        for part in range(2):
            pad_weights(part, 0)

    def norm_chunk(slot, c):
        at = pl.ds(pl.multiple_of(slot * tok + c * NORM_ROWS, 16), NORM_ROWS)
        block = xin[slot, rows_at(c), :].astype(jnp.float32)
        xn[at, :] = normalize(block, pg_ref[...], ps_ref[...]).astype(HALF)

    def side(zp, c):
        @pl.when(mine)
        def _():
            for dy in range(1, across):
                token_y_in(zp, dy, c).wait_recv()
                token_s(side_slot(zp, dy), c).start()

        @pl.when(others)
        def _():
            for dy in range(1, across):
                token_s(side_slot(zp, dy), c).wait_recv()

    def norm_side(zp, c):
        for dy in range(1, across):
            norm_chunk(side_slot(zp, dy), c)

    def far(zp, c):
        slot = zp * across + y

        @pl.when(mine)
        def _():
            token_z_in(zp, c).wait_recv()
            for dy in range(1, across):
                token_y(zp, dy, c).start()
            token_s(slot, c).start()

        @pl.when(others)
        def _():
            token_s(slot, c).wait_recv()

    def q_relay(part):
        for j in range(1, pairs):
            for cc in range(2):
                q_x_in(part, j, cc).wait_recv()
                q_z(part, j, cc).start()

    @pl.when(mine)
    def _():
        xin[s] = tok_ref[z % images]

    @pl.when(others)
    def _():
        for c in range(chunks):
            token_s(s, c).wait_recv()

    for c in range(chunks):
        norm_chunk(s, c)
    for c in range(chunks):
        side(z, c)
        norm_side(z, c)
    pad_own()
    for c in range(chunks):
        for zp in z_order[1:]:
            far(zp, c)
        if c == 0:
            q_relay(0)
        if c:
            for zp in z_order[1:]:
                side(zp, c - 1)
        for zp in z_order[1:]:
            norm_chunk(zp * across + y, c)
            if c:
                norm_side(zp, c - 1)
    for step, zp in enumerate(z_order[1:]):
        side(zp, chunks - 1)
        if step == 1:
            pass_first(0)
        norm_side(zp, chunks - 1)

    for k in range(3):
        w_own(k).start()
        w_so(k).start()

    block_rows = across * tok

    def project(part):
        def one(i, carry):
            at = pl.ds(pl.multiple_of(i * block_rows, 16), block_rows)
            result = jnp.dot(xn[at, :], wbuf[part], preferred_element_type=jnp.float32) + bpad[part]
            packed[part, at, :] = result.astype(HALF)
            return carry

        lax.fori_loop(0, groups, one, 0)

    merge = 2 if 2 * block_rows <= 640 else 1

    def put_context(part, rows, sp, store):
        low, high = plan.sends[part]
        known = rows
        start = part * plan.span
        if part:
            known = jnp.concatenate([kept[sp], rows], axis=-1)
            start = 0
        for tile in range(plan.full):
            if low <= tile * tok < high:
                at = tile * LANES - start
                store(pl.ds(tile * tok, tok), known[:, at : at + LANES])
        if part and plan.rest:
            last = known[:, plan.full * LANES :]
            if plan.fold == 2:
                last = jnp.concatenate([last[: tok // 2], last[tok // 2 :]], axis=-1)
            else:
                last = jnp.concatenate([last, jnp.zeros((tok, LANES - plan.rest), HALF)], axis=-1)
            store(pl.ds(plan.full * tok, tok // plan.fold), last)

    def attend(part):
        def one(step, carry):
            if merge == 2:
                zp = (z - z % 2 + 2 * (1 - step)) % groups
            else:
                near = (step + 1) // 2 % 2
                far = 1 - step // 2
                zp = (z + near * (1 - 2 * (z % 2)) + 2 * far) % groups
            at = pl.ds(pl.multiple_of(zp * block_rows, 16), merge * block_rows)
            outs = []
            for h in range(plan.part_heads):
                base = h * 3 * LANES
                queries = packed[part, at, base : base + LANES]
                key_rows = packed[part, :, base + LANES : base + 2 * LANES]
                value_rows = packed[part, :, base + 2 * LANES : base + 3 * LANES]
                scores = lax.dot_general(
                    queries, key_rows, (((1,), (1,)), ((), ())), preferred_element_type=jnp.float32
                )
                highest = jnp.max(scores, axis=-1, keepdims=True)
                weights = jnp.exp2((scores - highest) * factor).astype(HALF)
                summed = jnp.dot(weights, value_rows, preferred_element_type=jnp.float32)
                outs.append(summed[:, :HEAD_DIM] / summed[:, HEAD_DIM : HEAD_DIM + 1])
            whole = (jnp.concatenate(outs, axis=-1) if len(outs) > 1 else outs[0]).astype(HALF)
            for yy in range(merge * across):
                sp = zp * across + yy
                rows = whole[yy * tok : (yy + 1) * tok]

                def to_mixed(run, values):
                    mixed[sp, run] = values

                put_context(part, rows, sp, to_mixed)
                own = jnp.logical_and(mine, sp == s)

                @pl.when(own)
                def _():
                    def to_landed(run, values):
                        landed[group, z % images, run] = values

                    put_context(part, rows, sp, to_landed)

                if sends_in(part):

                    @pl.when(jnp.logical_not(own))
                    def _():
                        ctx_copy(part, sp, group, z % images).start()

                if part == 0:
                    kept[sp] = rows

            return carry

        lax.fori_loop(0, groups // merge, one, 0)

    pad_others(0)
    for part in range(1, n_parts):
        q_relay(part)
    project(0)
    attend(0)
    pass_first(1)
    pad_others(1)
    project(1)
    attend(1)
    pass_first(2)
    pass_first(3)
    pass_first(4)

    def context_in(part, gg, i):
        if not sends_in(part):
            return
        yy, cc = gg // 2, gg % 2
        source = (core * images + i) * across + yy
        own = jnp.logical_and(source == s, core == cc)
        low, high = plan.sends[part]
        slot = landed.at[gg, i, pl.ds(low, high - low)]

        @pl.when(jnp.logical_not(own))
        def _():
            remote(
                slot, slot, c_send.at[part, 0], c_recv.at[part, gg, i], (pair * 2 + cc, source)
            ).wait_recv()

    def contexts_in(part):
        for i in range(images):
            for gg in range(2 * across):
                context_in(part, gg, i)

    def gather_contexts():
        columns = plan.heads * HEAD_DIM
        for i in range(images):
            for gg in range(2 * across):
                cut = [landed[gg, i, t * tok : (t + 1) * tok] for t in range(plan.full)]
                if plan.rest:
                    last = landed[gg, i, plan.full * tok : plan.ctx_rows]
                    if plan.fold == 2:
                        last = jnp.concatenate([last[:, : plan.rest], last[:, plan.rest :]], axis=0)
                    cut.append(last[:, : plan.rest])
                ctx[i * tok : (i + 1) * tok, gg * columns : (gg + 1) * columns] = jnp.concatenate(cut, axis=-1)

    contexts_in(0)
    pass_second(0)
    pass_second(1)
    pass_first(5)
    contexts_in(1)
    gather_contexts()
    arrived(0)
    row_count = images * tok

    def project_out(c, carry):
        cols = pl.ds(pl.multiple_of(c * (plan.width // 2), LANES), plan.width // 2)
        attended = jnp.dot(ctx[...], w_out[:, cols], preferred_element_type=jnp.float32)
        residual = tok_ref[:, :, cols].astype(jnp.float32).reshape(row_count, plan.width // 2)
        mid[:, cols] = residual + attended + ob_ref[:, cols]
        return carry

    lax.fori_loop(0, 2, project_out, 0)

    def second_norm(i, carry):
        at = pl.ds(pl.multiple_of(i * NORM_ROWS, 16), NORM_ROWS)
        ctx[at, :] = normalize(mid[at, :], mg_ref[...], ms_ref[...]).astype(HALF)
        return carry

    lax.fori_loop(0, row_count // NORM_ROWS, second_norm, 0)

    def lift(cols):
        lifted = jnp.dot(ctx[...], w_up[:, cols], preferred_element_type=jnp.float32)
        lifted = lifted + ub_ref[:, cols]
        hid[:, cols] = (0.5 * lifted * (1.0 + lax.erf(lifted * math.sqrt(0.5)))).astype(HALF)

    def piece_in(q, second):
        for j in range(1, pairs):
            w_s(q, j, second, True).wait_recv()

    def run_columns(first, last, second):
        k, low, _, along_z = pieces[first]
        columns = pieces[last][1] + pieces[last][2] - low
        return piece_columns((k, low, columns, along_z), second)

    w_own(1).wait()
    w_so(1, True).wait_recv()
    for q in (1, 2, 3, 4):
        piece_in(q, False)
    lift(run_columns(1, 1, False))
    lift(run_columns(2, 3, False))
    lift(run_columns(4, 4, False))
    pass_first(6)
    pass_second(2)
    pass_second(3)
    piece_in(1, True)
    piece_in(2, True)
    lift(run_columns(1, 2, True))
    pass_first(7)
    pass_second(4)
    piece_in(3, True)
    lift(run_columns(3, 3, True))
    piece_in(4, True)
    lift(run_columns(4, 4, True))

    def result_copy(slot, cols):
        return pltpu.make_async_copy(o_ref.at[:, :, cols], o_out.at[:, :, cols], io_sem.at[slot + 1])

    def lower(slot, cols):
        lowered = jnp.dot(hid[...], w_down[:, cols], preferred_element_type=jnp.float32)
        result = (mid[:, cols] + lowered + db_ref[:, cols]).astype(HALF)
        o_ref[:, :, cols] = result.reshape(images, tok, cols.size)
        result_copy(slot, cols).start()

    w_own(2).wait()
    w_so(2, True).wait_recv()
    lowered_runs = ((5, 5, False), (6, 6, False), (7, 7, False), (5, 5, True), (6, 6, True), (7, 7, True))
    pass_second(5)
    for q in (5, 6, 7):
        piece_in(q, False)
    for slot in range(3):
        lower(slot, run_columns(*lowered_runs[slot]))
    pass_second(6)
    piece_in(5, True)
    lower(3, run_columns(*lowered_runs[3]))
    pass_second(7)
    for slot in (4, 5):
        piece_in(slot + 2, True)
        lower(slot, run_columns(*lowered_runs[slot]))

    def results_out():
        for slot in range(6):
            result_copy(slot, run_columns(*lowered_runs[slot])).wait()

    results_out()

    def drain():
        for c in range(chunks):
            for k in range(images):

                @pl.when(core * images + k != z)
                def _():
                    token_z(k, c).wait_send()

            @pl.when(mine)
            def _():
                for zp in range(groups):
                    for dy in range(1, across):
                        token_y(zp, dy, c).wait_send()
                for sp in range(n):
                    token_s(sp, c).wait_send()

        for part in range(n_parts):
            q_s(part).wait_send()
            for j in range(1, pairs):
                for cc in range(2):
                    q_x(part, j, cc).wait_send()
                    q_z(part, j, cc).wait_send()
        for k in range(3):
            w_so(k).wait_send()
        for q in range(len(pieces)):
            for j in range(1, pairs):
                w_x(q, j).wait_send()
                w_p(q, j).wait_send()
                w_s(q, j, False).wait_send()
                w_s(q, j, True).wait_send()
        for part in range(2):
            for sp in range(n):

                @pl.when(jnp.logical_not(jnp.logical_and(mine, sp == s)))
                def _():
                    if sends_in(part):
                        ctx_copy(part, sp, group, z % images).wait_send()

    drain()


def shards(n, n_dp, tokens, pre_gain, pre_shift, w_qkv, qkv_bias, w_out, out_bias, mlp_gain, mlp_shift,
           w_up, up_bias, w_down, down_bias):
    images, tok, width = tokens.shape
    hidden = w_up.shape[1]
    plan = Plan(n, n_dp, images, tok, width, hidden, w_qkv.shape[1])
    rows = images * tok
    dma = pltpu.SemaphoreType.DMA
    anywhere = pl.BlockSpec(memory_space=pl.ANY)
    pairs, groups, across = plan.pairs, plan.groups, plan.across
    n_pieces = len(pieces_of(plan))
    parts = len(plan.cuts) - 1
    chunks = tok // NORM_ROWS
    vectors = (pre_gain, pre_shift, qkv_bias, out_bias, mlp_gain, mlp_shift, up_bias, down_bias)
    return pl.pallas_call(
        functools.partial(layer_kernel, plan),
        out_shape=jax.ShapeDtypeStruct(tokens.shape, HALF),
        in_specs=[anywhere] * 13,
        out_specs=anywhere,
        scratch_shapes=[
            pltpu.VMEM(tokens.shape, HALF),
            pltpu.VMEM(tokens.shape, HALF),
            dma((1 + 2 * n_pieces,)),
            *[pltpu.VMEM((1, v.shape[0]), jnp.float32) for v in vectors],
            dma((8,)),
            pltpu.VMEM((n, tok, width), HALF),
            pltpu.VMEM((plan.length, width), HALF),
            pltpu.VMEM((width, plan.window), HALF),
            pltpu.VMEM((2, width, plan.part_columns), HALF),
            pltpu.VMEM((2, 1, plan.part_columns), jnp.float32),
            pltpu.VMEM((2, plan.length, plan.part_columns), HALF),
            pltpu.VMEM((n, tok, plan.span), HALF),
            pltpu.VMEM((n, plan.ctx_rows, LANES), HALF),
            pltpu.VMEM((2 * across, images, plan.ctx_rows, LANES), HALF),
            pltpu.VMEM((rows, width), HALF),
            pltpu.VMEM((rows, width), jnp.float32),
            pltpu.VMEM((rows, hidden), HALF),
            pltpu.VMEM((width, width), HALF),
            pltpu.VMEM((width, hidden), HALF),
            pltpu.VMEM((hidden, width), HALF),
            dma((images, chunks)),
            dma((groups, chunks)),
            dma((groups, across, chunks)),
            dma((groups, across, chunks)),
            dma((n, chunks)),
            dma((n, chunks)),
            dma((parts, pairs, 2)),
            dma((parts, pairs, 2)),
            dma((parts, pairs, 2)),
            dma((parts, pairs, 2)),
            dma((parts,)),
            dma((parts,)),
            dma((parts,)),
            dma((n_pieces, pairs)),
            dma((n_pieces, pairs)),
            dma((n_pieces, pairs)),
            dma((n_pieces, pairs)),
            dma((n_pieces, pairs, 2)),
            dma((n_pieces, pairs, 2)),
            dma((3,)),
            dma((3,)),
            dma((3,)),
            dma((2, n)),
            dma((2, 2 * across, images)),
        ],
        compiler_params=pltpu.CompilerParams(
            collective_id=0, has_side_effects=True, vmem_limit_bytes=67043328
        ),
        name="encoder_layer",
    )(
        tokens,
        w_qkv,
        w_out,
        w_up,
        w_down,
        *vectors,
    )


def solution(mesh):
    in_specs = (
        P("dp", "seq", None),
        P(),
        P(),
        P("dp", None),
        P(),
        P("dp", None),
        P(),
        P(),
        P(),
        P("dp", None),
        P(),
        P("dp", None),
        P(),
    )
    out_specs = P("dp", "seq", None)
    step = functools.partial(shards, mesh.shape["seq"], mesh.shape["dp"])
    return jax.shard_map(step, mesh=mesh, in_specs=in_specs, out_specs=out_specs, check_vma=False)
```
